256 devices in a mesh: cp: 64 (over z_hi, y, x), sp: 4 (over z_lo, core).
Axes of the slice: x: 4, y: 4, z: 8 (z_hi: 4, z_lo: 2; z = z_hi * 2 + z_lo), core: 2. Of those that a mesh axis runs over, the one named last changes fastest.
Arguments:
- queries: bfloat16 [24576, 2048], P(('cp', 'sp')), may hold values from -6 to 6
- key_vectors: bfloat16 [24576, 512], P(('cp', 'sp')), may hold values from -6 to 6
- value_matrix: bfloat16 [24576, 512], P(('cp', 'sp')), may hold values from -6 to 6
- span_order: int32 [64], replicated, may hold values from 0 to 63, each once
Outputs:
- attended: bfloat16 [24576, 2048], P(('cp', 'sp'))
The draws below stay inside these ranges and needn't reach their ends.
Inputs may be any that keep to these rules, and one draw needn't show every extreme that they name: `span_order`: each value appears exactly once.
All inputs are finite; a program needn't handle non-finite values.
Results may differ from the reference program's by a relative error of at most 0.0055.
Values may be sent and summed in bfloat16 or wider, within the bound.
No kernel may reach another device: no remote copies, remote signals or barrier semaphores. Data moves between devices by JAX's collectives and lax.ppermute only.
A program may use at most 128 MiB of HBM per device.

```python
import jax
import jax.numpy as jnp
from jax import lax

QUERY_HEADS = 16
KEY_VALUE_HEADS = 4
HEAD_WIDTH = 128
TOK_DEV = 96
SEQUENCE_TOKENS = 24576
PAIRS = 64
N_CP = 64
N_SP = 4


def drawn_pair(key):
    key_query, key_seed = jax.random.split(key, 2)
    query_draw = jnp.clip(jax.random.normal(key_query, (SEQUENCE_TOKENS, QUERY_HEADS * HEAD_WIDTH), jnp.float32), -6.0, 6.0)
    key_sample = jnp.clip(jax.random.normal(key_seed, (SEQUENCE_TOKENS, KEY_VALUE_HEADS * HEAD_WIDTH), jnp.float32), -6.0, 6.0)
    return (query_draw.astype(jnp.bfloat16), key_sample.astype(jnp.bfloat16))


def draw_queries(key, part):
    return drawn_pair(jax.random.fold_in(key, 11))[0]


def draw_key_vectors(key, part):
    return drawn_pair(jax.random.fold_in(key, 11))[1]


def block_scale(rng, dims, shards, low, high):
    def one(axis_at, blocks):
        steps = jax.random.uniform(jax.random.fold_in(jax.random.fold_in(rng, 6), axis_at), (blocks,), jnp.float32, low / len(shards), high / len(shards))
        return jnp.repeat(jnp.exp(steps), dims[axis_at] // blocks).reshape((-1,) + (1,) * (len(dims) - axis_at - 1))

    level = one(*shards[0])
    for cut in shards[1:]:
        level = level * one(*cut)
    return level


def gaussian(key, shape, spread, limit, shards=(), kind=jnp.bfloat16):
    result = jax.random.normal(key, shape, jnp.float32) * spread
    if len(shards) > 0:
        result = block_scale(key, shape, shards, -0.22, 0.18) * result
    return jnp.clip(result, min=-limit, max=limit).astype(kind)


def setup_inputs(seed: int = 0) -> dict:
    seeds = jax.random.split(jax.random.key(seed), 5)
    queries = draw_queries(jax.random.fold_in(seeds[4], 71), 0)
    key_vectors = draw_key_vectors(jax.random.fold_in(seeds[4], 71), 0)
    value_matrix = gaussian(seeds[2], (SEQUENCE_TOKENS, KEY_VALUE_HEADS * HEAD_WIDTH), 1.0, 6.0, ((0, 256),))
    span_order = jax.random.permutation(seeds[3], PAIRS).astype(jnp.int32)
    return {"queries": queries, "key_vectors": key_vectors, "value_matrix": value_matrix, "span_order": span_order}


def span_position(row_ids, span_order, pair_count, span_rows):
    slot_ids = row_ids // span_rows
    pair_ids = slot_ids // 2
    picked = jnp.sum(jnp.where(pair_ids[:, None] == jnp.arange(pair_count, dtype=jnp.int32)[None, :], span_order[None, :], 0), axis=1).astype(jnp.int32)
    span_ids = jnp.where(slot_ids % 2 == 1, 2 * pair_count - 1 - picked, picked)
    return (span_ids * span_rows + row_ids % span_rows).astype(jnp.int32)


def reference(queries, key_vectors, value_matrix, span_order):
    total_rows = queries.shape[0]
    span_rows = TOK_DEV * N_SP // 2
    row_ids = jnp.arange(total_rows, dtype=jnp.int32)
    positions = span_position(row_ids, span_order, N_CP, span_rows)
    group_width = QUERY_HEADS // KEY_VALUE_HEADS
    block_row_list = 512 if total_rows % 512 == 0 else total_rows
    block_total = total_rows // block_row_list
    entry_list = jnp.arange(block_total * KEY_VALUE_HEADS, dtype=jnp.int32)

    def attend(single_entry):
        block_number = single_entry // KEY_VALUE_HEADS
        key_value_head = single_entry % KEY_VALUE_HEADS
        first_row = (block_number * block_row_list).astype(jnp.int32)
        query_blk = lax.dynamic_slice(queries, (first_row, (key_value_head * group_width * HEAD_WIDTH).astype(jnp.int32)), (block_row_list, group_width * HEAD_WIDTH))
        query_blk = query_blk.astype(jnp.float32).reshape(block_row_list, group_width, HEAD_WIDTH)
        key_blk = lax.dynamic_slice(key_vectors, (jnp.int32(0), (key_value_head * HEAD_WIDTH).astype(jnp.int32)), (total_rows, HEAD_WIDTH)).astype(jnp.float32)
        value_blk = lax.dynamic_slice(value_matrix, (jnp.int32(0), (key_value_head * HEAD_WIDTH).astype(jnp.int32)), (total_rows, HEAD_WIDTH)).astype(jnp.float32)
        query_pos = lax.dynamic_slice(positions, (first_row,), (block_row_list,))
        scores = jnp.einsum("qhd,kd->hqk", query_blk, key_blk) * (HEAD_WIDTH ** -0.5)
        allowed = positions[None, None, :] <= query_pos[None, :, None]
        row_max = jnp.max(jnp.where(allowed, scores, -1e30), axis=2)
        weights = jnp.where(allowed, jnp.exp(scores - row_max[:, :, None]), 0.0)
        row_sum = jnp.sum(weights, axis=2)
        rounded = lax.optimization_barrier(weights.astype(jnp.bfloat16)).astype(jnp.float32)
        summed = jnp.einsum("hqk,kd->qhd", rounded, value_blk)
        return (summed / jnp.transpose(row_sum)[:, :, None]).astype(jnp.bfloat16)

    output_list = lax.map(attend, entry_list)
    output_list = output_list.reshape(block_total, KEY_VALUE_HEADS, block_row_list, group_width, HEAD_WIDTH)
    return jnp.transpose(output_list, (0, 2, 1, 3, 4)).reshape(total_rows, QUERY_HEADS * HEAD_WIDTH)
```

```python
import jax
import jax.numpy as jnp
from jax import lax
from jax.experimental import pallas as pl
from jax.experimental.pallas import tpu as pltpu
from jax.sharding import Mesh
from jax.sharding import PartitionSpec as P

D = 128
HEADS = 4
AXES = ("zh", "y", "x", "zl", "c")
LOG2E = 1.4426950408889634
LOW = -1e30
NB = 5
CHUNKS = 2
ROWS_O = 136
VMEM = pl.BlockSpec(memory_space=pltpu.VMEM)
SMEM = pl.BlockSpec(memory_space=pltpu.SMEM)


def params():
    return pltpu.CompilerParams(vmem_limit_bytes=48 * 1024 * 1024)


def prep_kernel(q_ref, out_ref):
    for h in range(4):
        cols = [q_ref[:, pl.ds((h * HEADS + j) * D, D)] for j in range(HEADS)]
        stacked = jnp.concatenate(cols, axis=0).astype(jnp.float32)
        out_ref[h] = jnp.transpose(stacked).astype(jnp.bfloat16)


def prep(queries):
    tok = queries.shape[0]
    return pl.pallas_call(
        prep_kernel,
        out_shape=jax.ShapeDtypeStruct((4, D, HEADS * tok), jnp.bfloat16),
        in_specs=[VMEM],
        out_specs=VMEM,
        compiler_params=params(),
        name="prep_q",
    )(queries)


def make_attend(first, last, piece_rows, span_rows, n_pieces, units):
    width = units[0]
    tiles = 2 * width // 256

    def kernel(*refs):
        tab, spans, nfull, nall, qspan, koff, tok, qa, qb, kv = refs[:10]
        rest = refs[10:]
        if not first:
            acc_in, m_in, l_in = rest[:3]
            rest = rest[3:]
        if last:
            own_ref, other_ref, acc, m, l = rest
        else:
            acc, m, l = rest

        def q_tile(j, t):
            lo = t * 256
            if lo + 256 <= width:
                return qa[j, :, lo : lo + 256]
            if lo >= width:
                return qb[j, :, lo - width : lo - width + 256]
            return jnp.concatenate([qa[j, :, lo:], qb[j, :, : 256 - (width - lo)]], axis=1)

        def block(j, base, masked):
            rows = [pl.ds(pl.multiple_of(tab[base + i] * piece_rows, 16), piece_rows) for i in range(NB)]
            keys = jnp.concatenate([kv[r, 0:D] for r in rows], axis=0)
            vals = jnp.concatenate([kv[r, D : 2 * D] for r in rows], axis=0)
            if masked:
                within = lax.broadcasted_iota(jnp.int32, (piece_rows, 256), 0) + koff[0]
                kpos = jnp.concatenate([within + spans[base + i] * span_rows for i in range(NB)], axis=0)
            for t in range(tiles):
                cs = pl.ds(t * 256, 256)
                s = jnp.dot(keys, q_tile(j, t), preferred_element_type=jnp.float32) * (LOG2E * D**-0.5)
                if masked:
                    ok = kpos <= tok[:, cs] + qspan[j] * span_rows
                    s = jnp.where(ok, s, LOW)
                m_old = m[j, :, cs]
                m_new = jnp.maximum(m_old, jnp.max(s, axis=0, keepdims=True))
                alpha = jnp.exp2(m_old - m_new)
                p = jnp.exp2(s - m_new)
                if masked:
                    p = jnp.where(ok, p, 0.0)
                l[j, :, cs] = l[j, :, cs] * alpha + jnp.sum(p, axis=0, keepdims=True)
                m[j, :, cs] = m_new
                pv = lax.dot_general(
                    vals, p.astype(jnp.bfloat16), (((0,), (0,)), ((), ())), preferred_element_type=jnp.float32
                )
                acc[j, :, cs] = acc[j, :, cs] * alpha + pv

        def one_span(j, carry):
            if first:
                acc[j] = jnp.zeros(acc.shape[1:], jnp.float32)
                m[j] = jnp.full(m.shape[1:], LOW, jnp.float32)
                l[j] = jnp.zeros(l.shape[1:], jnp.float32)
            else:
                acc[j] = acc_in[j]
                m[j] = m_in[j]
                l[j] = l_in[j]
            full = nfull[j] // NB

            def step(b, c):
                block(j, b * NB, False)
                return c

            lax.fori_loop(0, full, step, 0)

            @pl.when(nall[j] > full * NB)
            def _():
                block(j, full * NB, True)

            if last:
                total = l[j]
                seen = total > 0.0
                safe = jnp.where(seen, total, 1.0)
                lse = jnp.where(seen, m[j] + jnp.log2(safe), LOW)
                inv = 1.0 / safe
                hi = lse.astype(jnp.bfloat16)
                r1 = lse - hi.astype(jnp.float32)
                mid = r1.astype(jnp.bfloat16)
                low = (r1 - mid.astype(jnp.float32)).astype(jnp.bfloat16)
                stat = jnp.concatenate(
                    [hi.astype(jnp.float32), mid.astype(jnp.float32), low.astype(jnp.float32), jnp.zeros((5, 2 * width), jnp.float32)], axis=0
                ).astype(jnp.bfloat16)
                for ref, lo in ((own_ref, 0), (other_ref, width)):
                    cs = pl.ds(lo, width)
                    ref[j, 0:D] = (acc[j, :, cs] * inv[:, lo : lo + width]).astype(jnp.bfloat16)
                    ref[j, D:ROWS_O] = stat[:, lo : lo + width]
            return carry

        lax.fori_loop(0, qa.shape[0], one_span, 0)

    return kernel


def attend(tables, qa, qb, kv, state, last, piece_rows, span_rows):
    first = state is None
    n_q, _, width = qa.shape
    state_shapes = [
        ((n_q, D, 2 * width), jnp.float32),
        ((n_q, 1, 2 * width), jnp.float32),
        ((n_q, 1, 2 * width), jnp.float32),
    ]
    if last:
        out_shape = [jax.ShapeDtypeStruct((n_q, ROWS_O, width), jnp.bfloat16)] * 2
        scratch = [pltpu.VMEM(s, d) for s, d in state_shapes]
    else:
        out_shape = [jax.ShapeDtypeStruct(s, d) for s, d in state_shapes]
        scratch = []
    args = list(tables) + [qa, qb, kv] + ([] if first else list(state))
    flops = 2 * 2 * n_q * 2 * width * D * kv.shape[0] // 2
    return pl.pallas_call(
        make_attend(first, last, piece_rows, span_rows, kv.shape[0] // piece_rows, (width,)),
        out_shape=out_shape,
        in_specs=[SMEM] * 6 + [VMEM] * (len(args) - 6),
        out_specs=[VMEM] * len(out_shape),
        scratch_shapes=scratch,
        compiler_params=params(),
        cost_estimate=pl.CostEstimate(flops=flops * 2, bytes_accessed=kv.size * 2, transcendentals=0),
        name="attend_last" if last else "attend_more",
    )(*args)


def weights_of(a, b):
    def lse(ref):
        return ref[D : D + 1].astype(jnp.float32) + ref[D + 1 : D + 2].astype(jnp.float32) + ref[D + 2 : D + 3].astype(jnp.float32)

    la, lb = lse(a), lse(b)
    top = jnp.maximum(la, lb)
    ea, eb = jnp.exp2(la - top), jnp.exp2(lb - top)
    total = ea + eb
    return ea / total, eb / total, top + jnp.log2(total)


def combine_kernel(a_ref, b_ref, keep_ref, send_ref):
    half = keep_ref.shape[0]
    for j in range(a_ref.shape[0]):
        wa, wb, lse = weights_of(a_ref[j], b_ref[j])
        mixed = a_ref[j, 0:D].astype(jnp.float32) * wa + b_ref[j, 0:D].astype(jnp.float32) * wb
        hi = lse.astype(jnp.bfloat16).astype(jnp.float32)
        mid = (lse - hi).astype(jnp.bfloat16).astype(jnp.float32)
        low = lse - hi - mid
        stat = jnp.concatenate([hi, mid, low, jnp.zeros((5, lse.shape[1]), jnp.float32)], axis=0)
        ref = keep_ref if j < half else send_ref
        ref[j % half, 0:D] = mixed.astype(jnp.bfloat16)
        ref[j % half, D:ROWS_O] = stat.astype(jnp.bfloat16)


def combine(a, b):
    n = a.shape[0] // 2
    shape = jax.ShapeDtypeStruct((n,) + a.shape[1:], jnp.bfloat16)
    return pl.pallas_call(
        combine_kernel,
        out_shape=[shape, shape],
        in_specs=[VMEM] * 2,
        out_specs=[VMEM] * 2,
        compiler_params=params(),
        name="combine_cores",
    )(a, b)


def finish_kernel(a_ref, b_ref, out_ref):
    tok = out_ref.shape[1]
    for j in range(a_ref.shape[0]):
        wa, wb, _ = weights_of(a_ref[j], b_ref[j])
        mixed = a_ref[j, 0:D].astype(jnp.float32) * wa + b_ref[j, 0:D].astype(jnp.float32) * wb
        rows = jnp.transpose(mixed).astype(jnp.bfloat16)
        for h in range(HEADS):
            out_ref[j, :, pl.ds(h * D, D)] = rows[h * tok : (h + 1) * tok]


def finish(a, b):
    tok = a.shape[2] // HEADS
    return pl.pallas_call(
        finish_kernel,
        out_shape=jax.ShapeDtypeStruct((a.shape[0], tok, HEADS * D), jnp.bfloat16),
        in_specs=[VMEM] * 2,
        out_specs=VMEM,
        compiler_params=params(),
        name="combine_chips",
    )(a, b)


def swap(x, axis):
    return lax.ppermute(x, axis, [(0, 1), (1, 0)])


def exchange(x, axes):
    return lax.all_to_all(x, axes, split_axis=0, concat_axis=0, tiled=True)


def per_device(queries, key_vectors, value_matrix, span_order):
    tok = queries.shape[0]
    pairs = span_order.shape[0]
    span_rows = 2 * tok
    piece = tok // 2
    yx = lax.axis_size("y") * lax.axis_size("x")
    zl, c = lax.axis_index("zl"), lax.axis_index("c")
    mine = lax.axis_index("y") * lax.axis_size("x") + lax.axis_index("x")

    kv = jnp.stack([key_vectors.reshape(tok, 4, D), value_matrix.reshape(tok, 4, D)], axis=2).reshape(2, piece, 4, 2 * D)
    kv = jnp.transpose(kv, (2, 0, 1, 3)).reshape(8, piece, 2 * D)
    column = exchange(kv, ("zh", "zl"))

    q_t = exchange(prep(queries), "zh")
    q_near = jnp.concatenate([q_t, swap(q_t, "zl")], axis=0)
    q_far = swap(q_near, "c")

    per = 8 // CHUNKS
    order = span_order.astype(jnp.int32).reshape(4, yx)
    piece_span = jnp.stack([order, 2 * pairs - 1 - order], axis=1).reshape(CHUNKS, per, yx)
    piece_span = jnp.transpose(piece_span, (0, 2, 1)).reshape(CHUNKS, per * yx)
    count = per * yx
    ids = jnp.arange(count, dtype=jnp.int32)
    rank = jnp.sum((piece_span[:, None, :] < piece_span[:, :, None]).astype(jnp.int32), axis=2)
    hit = rank[:, None, :] == ids[None, :, None]
    tab = jnp.sum(jnp.where(hit, ids[None, None, :], 0), axis=2)
    spans = jnp.sum(jnp.where(hit, piece_span[:, None, :], 0), axis=2)
    tab = jnp.pad(tab, ((0, 0), (0, NB)))
    spans = jnp.pad(spans, ((0, 0), (0, NB)), constant_values=1 << 16)
    here = jnp.sum(jnp.where(jnp.arange(yx, dtype=jnp.int32)[None, :] == mine, order, 0), axis=1)
    early, late = here, 2 * pairs - 1 - here
    q_span = jnp.concatenate([jnp.where(zl == 0, early, late), jnp.where(zl == 0, late, early)])
    nfull = jnp.sum((piece_span[:, None, :] < q_span[None, :, None]).astype(jnp.int32), axis=2)
    nall = jnp.sum((piece_span[:, None, :] <= q_span[None, :, None]).astype(jnp.int32), axis=2)
    koff = (c * tok + zl * piece).astype(jnp.int32).reshape(1)
    cols = jnp.arange(2 * HEADS * tok, dtype=jnp.int32)
    side = jnp.where(cols < HEADS * tok, c, 1 - c)
    token = (cols % tok + side * tok).astype(jnp.int32)[None, :]

    state = None
    for k in range(CHUNKS):
        rows = column[k * per : (k + 1) * per].reshape(1, per * piece, 2 * D)
        gathered = exchange(jnp.broadcast_to(rows, (yx, per * piece, 2 * D)), ("y", "x"))
        gathered = gathered.reshape(yx * per * piece, 2 * D)
        tables = (tab[k], spans[k], nfull[k], nall[k], q_span, koff)
        state = attend(tables + (token,), q_near, q_far, gathered, state, k == CHUNKS - 1, piece, span_rows)
    own, other = state
    keep, send = combine(own, swap(other, "c"))
    done = finish(keep, swap(send, "zl"))
    back = exchange(done, "zh")
    return jnp.transpose(back, (1, 0, 2)).reshape(tok, 4 * HEADS * D)


def solution(mesh):
    finer = Mesh(mesh.devices.reshape(4, 4, 4, 2, 2), AXES)
    spec = P(AXES, None)
    return jax.shard_map(
        per_device, mesh=finer, in_specs=(spec, spec, spec, P()), out_specs=spec, check_vma=False
    )
```

```python
import jax
import jax.numpy as jnp
from jax import lax
from jax.experimental import pallas as pl
from jax.experimental.pallas import tpu as pltpu
from jax.sharding import Mesh
from jax.sharding import PartitionSpec as P

D = 128
HEADS = 4
AXES = ("zh", "y", "x", "zl", "c")
LOG2E = 1.4426950408889634
LOW = -1e30
SCALE = LOG2E * D**-0.5
NB = 5
ROWS_O = 136
GROUPS = ((1, 2), (3,), (0,))
VMEM = pl.BlockSpec(memory_space=pltpu.VMEM)
SMEM = pl.BlockSpec(memory_space=pltpu.SMEM)


def params(mib=20):
    return pltpu.CompilerParams(vmem_limit_bytes=mib * 1024 * 1024)


def split_kernel(k_ref, v_ref, out_ref):
    half = out_ref.shape[1]
    for h in range(4):
        for part in range(2):
            rows = pl.ds(part * half, half)
            out_ref[2 * h + part, :, 0:D] = k_ref[rows, pl.ds(h * D, D)]
            out_ref[2 * h + part, :, D : 2 * D] = v_ref[rows, pl.ds(h * D, D)]


def split_heads(keys, values):
    return pl.pallas_call(
        split_kernel,
        out_shape=jax.ShapeDtypeStruct((8, keys.shape[0] // 2, 2 * D), jnp.bfloat16),
        in_specs=[VMEM] * 2,
        out_specs=VMEM,
        compiler_params=params(),
        name="split_heads",
    )(keys, values)


def turn_kernel(at_ref, q_ref, *out_refs):
    for k, out_ref in enumerate(out_refs):
        head = lax.rem(at_ref[0] + k, 4) * HEADS
        cols = [q_ref[:, pl.ds(pl.multiple_of((head + j) * D, D), D)] for j in range(HEADS)]
        stacked = jnp.concatenate(cols, axis=0).astype(jnp.float32)
        out_ref[...] = jnp.transpose(stacked).astype(jnp.bfloat16)


def turn(at, queries):
    tok = queries.shape[0]
    return pl.pallas_call(
        turn_kernel,
        out_shape=[jax.ShapeDtypeStruct((D, HEADS * tok), jnp.bfloat16)] * 4,
        in_specs=[SMEM, VMEM],
        out_specs=[VMEM] * 4,
        compiler_params=params(),
        name="turn_queries",
    )(at, queries)


def place_kernel(at_ref, *refs):
    out_ref = refs[4]
    width = HEADS * D
    for k in range(4):
        head = lax.rem(at_ref[0] + k, 4)
        out_ref[:, pl.ds(pl.multiple_of(head * width, width), width)] = refs[k][...]


def place(at, blocks):
    tok = blocks[0].shape[0]
    return pl.pallas_call(
        place_kernel,
        out_shape=jax.ShapeDtypeStruct((tok, 4 * HEADS * D), jnp.bfloat16),
        in_specs=[SMEM] + [VMEM] * 4,
        out_specs=VMEM,
        compiler_params=params(),
        name="place_heads",
    )(at, *blocks)


def make_attend(first_unit, units, piece_rows, span_rows, count, width):
    tiles = 2 * width // 256
    tok = span_rows // 2
    padded = count + 2 * NB

    def kernel(table, qa, qb, kv, own_ref, other_ref, acc, m, l, s0, s1, t0, t1):
        at_tab, at_span, at_full, at_all, at_q = 0, padded, 2 * padded, 2 * padded + 8, 2 * padded + 16
        koff, near, away = table[2 * padded + 24], table[2 * padded + 25], table[2 * padded + 26]

        def q_tile(j, t):
            lo = t * 256
            if lo + 256 <= width:
                return qa[j, :, lo : lo + 256]
            if lo >= width:
                return qb[j, :, lo - width : lo - width + 256]
            return jnp.concatenate([qa[j, :, lo:], qb[j, :, : 256 - (width - lo)]], axis=1)

        def rows_of(base):
            return [
                pl.ds(pl.multiple_of(table[at_tab + base + i] * piece_rows, 16), piece_rows) for i in range(NB)
            ]

        def score(j, base, s_ref, top_ref):
            keys = jnp.concatenate([kv[r, 0:D] for r in rows_of(base)], axis=0)
            for t in range(tiles):
                cs = pl.ds(t * 256, 256)
                s = jnp.dot(keys, q_tile(j, t), preferred_element_type=jnp.float32)
                s_ref[:, cs] = s
                top_ref[:, cs] = jnp.max(s, axis=0, keepdims=True)

        def absorb(j, base, s_ref, top_ref, masked):
            vals = jnp.concatenate([kv[r, D : 2 * D] for r in rows_of(base)], axis=0)
            if masked:
                within = lax.broadcasted_iota(jnp.int32, (piece_rows, 256), 0) + koff
                kpos = jnp.concatenate(
                    [within + table[at_span + base + i] * span_rows for i in range(NB)], axis=0
                )
            for t in range(tiles):
                cs = pl.ds(t * 256, 256)
                s = s_ref[:, cs]
                if masked:
                    col = lax.broadcasted_iota(jnp.int32, (1, 256), 1) + t * 256
                    qpos = lax.rem(col, tok) + jnp.where(col < width, near, away) + table[at_q + j] * span_rows
                    ok = kpos <= qpos
                    s = jnp.where(ok, s, LOW)
                    top = jnp.max(s, axis=0, keepdims=True)
                else:
                    top = top_ref[:, cs]
                m_old = m[:, cs]
                m_new = jnp.maximum(m_old, top * SCALE)
                alpha = jnp.exp2(m_old - m_new)
                p = jnp.exp2(s * SCALE - m_new)
                if masked:
                    p = jnp.where(ok, p, 0.0)
                l[:, cs] = l[:, cs] * alpha + jnp.sum(p, axis=0, keepdims=True)
                m[:, cs] = m_new
                pv = lax.dot_general(
                    vals, p.astype(jnp.bfloat16), (((0,), (0,)), ((), ())), preferred_element_type=jnp.float32
                )
                acc[:, cs] = acc[:, cs] * alpha + pv

        def one_span(u, carry):
            j = u + first_unit
            acc[...] = jnp.zeros(acc.shape, jnp.float32)
            m[...] = jnp.full(m.shape, LOW, jnp.float32)
            l[...] = jnp.zeros(l.shape, jnp.float32)
            full = table[at_full + j] // NB
            score(j, 0, s0, t0)

            def step(i, c):
                base = i * (2 * NB)
                score(j, base + NB, s1, t1)
                absorb(j, base, s0, t0, False)
                score(j, base + 2 * NB, s0, t0)
                absorb(j, base + NB, s1, t1, False)
                return c

            lax.fori_loop(0, full // 2, step, 0)
            odd = full % 2 == 1

            @pl.when(odd)
            def _():
                score(j, full * NB, s1, t1)
                absorb(j, full * NB - NB, s0, t0, False)
                absorb(j, full * NB, s1, t1, True)

            @pl.when(jnp.logical_not(odd))
            def _():
                absorb(j, full * NB, s0, t0, True)

            total = l[...]
            seen = total > 0.0
            safe = jnp.where(seen, total, 1.0)
            lse = jnp.where(seen, m[...] + jnp.log2(safe), LOW)
            inv = 1.0 / safe
            hi = lse.astype(jnp.bfloat16).astype(jnp.float32)
            mid = (lse - hi).astype(jnp.bfloat16).astype(jnp.float32)
            stat = jnp.concatenate([hi, mid, lse - hi - mid, jnp.zeros((5, 2 * width), jnp.float32)], axis=0)
            stat = stat.astype(jnp.bfloat16)
            for ref, lo in ((own_ref, 0), (other_ref, width)):
                cs = pl.ds(lo, width)
                ref[u, 0:D] = (acc[:, cs] * inv[:, lo : lo + width]).astype(jnp.bfloat16)
                ref[u, D:ROWS_O] = stat[:, lo : lo + width]
            return carry

        lax.fori_loop(0, units, one_span, 0)

    return kernel


def attend(table, qa, qb, kv, piece_rows, span_rows, group, first, units):
    width = qa.shape[2]
    count = kv.shape[0] // piece_rows
    wide = 2 * width
    flops = 2 * 2 * units * wide * D * kv.shape[0] // 2
    return pl.pallas_call(
        make_attend(first, units, piece_rows, span_rows, count, width),
        out_shape=[jax.ShapeDtypeStruct((units, ROWS_O, width), jnp.bfloat16)] * 2,
        in_specs=[SMEM] + [VMEM] * 3,
        out_specs=[VMEM] * 2,
        scratch_shapes=[
            pltpu.VMEM((D, wide), jnp.float32),
            pltpu.VMEM((1, wide), jnp.float32),
            pltpu.VMEM((1, wide), jnp.float32),
            pltpu.VMEM((NB * piece_rows, wide), jnp.float32),
            pltpu.VMEM((NB * piece_rows, wide), jnp.float32),
            pltpu.VMEM((1, wide), jnp.float32),
            pltpu.VMEM((1, wide), jnp.float32),
        ],
        compiler_params=params(),
        cost_estimate=pl.CostEstimate(flops=flops * 2, bytes_accessed=kv.size * 2, transcendentals=0),
        name="attend" + str(group),
    )(table, qa, qb, kv)


def weights_of(a, b):
    def lse(ref):
        s = ref[D : D + 8].astype(jnp.float32)
        return s[0:1] + s[1:2] + s[2:3]

    la, lb = lse(a), lse(b)
    top = jnp.maximum(la, lb)
    ea, eb = jnp.exp2(la - top), jnp.exp2(lb - top)
    total = ea + eb
    return ea / total, eb / total, top + jnp.log2(total)


def combine_kernel(a_ref, b_ref, keep_ref, send_ref):
    half = keep_ref.shape[0]
    for j in range(a_ref.shape[0]):
        wa, wb, lse = weights_of(a_ref[j], b_ref[j])
        mixed = a_ref[j, 0:D].astype(jnp.float32) * wa + b_ref[j, 0:D].astype(jnp.float32) * wb
        hi = lse.astype(jnp.bfloat16).astype(jnp.float32)
        mid = (lse - hi).astype(jnp.bfloat16).astype(jnp.float32)
        stat = jnp.concatenate([hi, mid, lse - hi - mid, jnp.zeros((5, lse.shape[1]), jnp.float32)], axis=0)
        ref = keep_ref if j < half else send_ref
        ref[j % half, 0:D] = mixed.astype(jnp.bfloat16)
        ref[j % half, D:ROWS_O] = stat.astype(jnp.bfloat16)


def combine(a, b):
    n = a.shape[0] // 2
    shape = jax.ShapeDtypeStruct((n,) + a.shape[1:], jnp.bfloat16)
    return pl.pallas_call(
        combine_kernel,
        out_shape=[shape, shape],
        in_specs=[VMEM] * 2,
        out_specs=[VMEM] * 2,
        compiler_params=params(),
        name="combine_cores",
    )(a, b)


def finish_kernel(a_ref, b_ref, *out_refs):
    tok = out_refs[0].shape[0]
    for j, out_ref in enumerate(out_refs):
        wa, wb, _ = weights_of(a_ref[j], b_ref[j])
        mixed = a_ref[j, 0:D].astype(jnp.float32) * wa + b_ref[j, 0:D].astype(jnp.float32) * wb
        rows = jnp.transpose(mixed).astype(jnp.bfloat16)
        for h in range(HEADS):
            out_ref[:, pl.ds(h * D, D)] = rows[h * tok : (h + 1) * tok]


def finish(a, b):
    tok = a.shape[2] // HEADS
    return pl.pallas_call(
        finish_kernel,
        out_shape=[jax.ShapeDtypeStruct((tok, HEADS * D), jnp.bfloat16)] * a.shape[0],
        in_specs=[VMEM] * 2,
        out_specs=[VMEM] * a.shape[0],
        compiler_params=params(),
        name="combine_chips",
    )(a, b)


def swap(x, axis):
    return lax.ppermute(x, axis, [(0, 1), (1, 0)])


def shift(x, k):
    return lax.ppermute(x, "zh", [(i, (i + k) % 4) for i in range(4)])


def exchange(x, axes):
    return lax.all_to_all(x, axes, split_axis=0, concat_axis=0, tiled=True)


def pick(values, index):
    slots = jnp.arange(values.shape[0], dtype=jnp.int32)
    return jnp.sum(jnp.where(slots[None, :] == index[:, None], values[None, :], 0), axis=1)


def per_device(queries, key_vectors, value_matrix, span_order):
    tok = queries.shape[0]
    pairs = span_order.shape[0]
    span_rows = 2 * tok
    piece = tok // 2
    yx = lax.axis_size("y") * lax.axis_size("x")
    zh, zl, c = (lax.axis_index(a).astype(jnp.int32) for a in ("zh", "zl", "c"))
    mine = lax.axis_index("y").astype(jnp.int32) * lax.axis_size("x") + lax.axis_index("x").astype(jnp.int32)
    at = jnp.stack([zh, zl])

    column = exchange(split_heads(key_vectors, value_matrix), ("zh", "zl"))
    blocks = turn(at, queries)
    spread = jnp.broadcast_to(column.reshape(1, 8 * piece, 2 * D), (yx, 8 * piece, 2 * D))
    spread, blocks = lax.optimization_barrier((spread, blocks))
    gathered = exchange(spread, ("y", "x")).reshape(yx * 8 * piece, 2 * D)

    got = [blocks[0]] + [shift(blocks[k], k) for k in range(1, 4)]
    far = swap(jnp.stack(got), "zl")
    q_near = jnp.stack([b for ks in GROUPS for b in [got[k] for k in ks] + [far[k] for k in ks]])
    q_far = swap(q_near, "c")

    order = span_order.astype(jnp.int32)
    span = jnp.arange(2 * pairs, dtype=jnp.int32)
    early = jnp.minimum(span, 2 * pairs - 1 - span)
    ids = jnp.arange(pairs, dtype=jnp.int32)
    pair = jnp.sum(jnp.where(order[None, :] == early[:, None], ids[None, :], 0), axis=1)
    tab = (pair % yx) * 8 + (pair // yx) * 2 + (span >= pairs)
    behind = (zh - jnp.asarray([k for ks in GROUPS for k in ks + ks], jnp.int32)) % 4
    other = jnp.asarray([f for ks in GROUPS for f in [0] * len(ks) + [1] * len(ks)], jnp.int32)
    here = pick(order, behind * yx + mine)
    q_span = jnp.where(zl == other, here, 2 * pairs - 1 - here)
    pad = jnp.zeros((2 * NB,), jnp.int32)
    scalars = jnp.stack([c * tok + zl * piece, c * tok, (1 - c) * tok])
    table = jnp.concatenate([tab, pad, span, pad + (1 << 16), q_span, q_span + 1, q_span, scalars])

    starts = [2 * sum(len(ks) for ks in GROUPS[:g]) for g in range(len(GROUPS))]
    ends, waiting = {}, []

    def merge(own, other):
        return combine(own, swap(other, "c"))

    def close(ks, keep, send):
        done = finish(keep, swap(send, "zl"))
        for i, k in enumerate(ks):
            ends[k] = done[i] if k == 0 else shift(done[i], 4 - k)

    merged = []
    for g, ks in enumerate(GROUPS):
        part = attend(table, q_near, q_far, gathered, piece, span_rows, g, starts[g], 2 * len(ks))
        waiting.append(part)
        if g == 0:
            table, waiting[0] = lax.optimization_barrier((table, part))
        elif g < len(GROUPS) - 1:
            merged.append(merge(*waiting.pop(0)))
            table, merged[-1], waiting[0] = lax.optimization_barrier((table, merged[-1], waiting[0]))
    merged += [merge(*w) for w in waiting]
    for ks, m in zip(GROUPS, merged):
        close(ks, *m)
    return place(at, [ends[k] for k in range(4)])


def solution(mesh):
    finer = Mesh(mesh.devices.reshape(4, 4, 4, 2, 2), AXES)
    spec = P(AXES, None)
    return jax.shard_map(
        per_device, mesh=finer, in_specs=(spec, spec, spec, P()), out_specs=spec, check_vma=False
    )
```

```python
import jax
import jax.numpy as jnp
from jax import lax
from jax.experimental import pallas as pl
from jax.experimental.pallas import tpu as pltpu
from jax.sharding import Mesh
from jax.sharding import PartitionSpec as P

D = 128
HEADS = 4
AXES = ("zh", "y", "x", "zl", "c")
LOG2E = 1.4426950408889634
LOW = -1e30
SCALE = LOG2E * D**-0.5
NB = 5
ROWS_O = 136
GROUPS = ((2,), (1,), (3,), (0,))
VMEM = pl.BlockSpec(memory_space=pltpu.VMEM)
SMEM = pl.BlockSpec(memory_space=pltpu.SMEM)


def params(mib=20):
    return pltpu.CompilerParams(vmem_limit_bytes=mib * 1024 * 1024)


def split_kernel(k_ref, v_ref, out_ref):
    half = out_ref.shape[1]
    for h in range(4):
        for part in range(2):
            rows = pl.ds(part * half, half)
            out_ref[2 * h + part, :, 0:D] = k_ref[rows, pl.ds(h * D, D)]
            out_ref[2 * h + part, :, D : 2 * D] = v_ref[rows, pl.ds(h * D, D)]


def split_heads(keys, values):
    return pl.pallas_call(
        split_kernel,
        out_shape=jax.ShapeDtypeStruct((8, keys.shape[0] // 2, 2 * D), jnp.bfloat16),
        in_specs=[VMEM] * 2,
        out_specs=VMEM,
        compiler_params=params(),
        name="split_heads",
    )(keys, values)


def turn_kernel(at_ref, q_ref, *out_refs):
    for k, out_ref in enumerate(out_refs):
        head = lax.rem(at_ref[0] + k, 4) * HEADS
        cols = [q_ref[:, pl.ds(pl.multiple_of((head + j) * D, D), D)] for j in range(HEADS)]
        stacked = jnp.concatenate(cols, axis=0).astype(jnp.float32)
        out_ref[...] = jnp.transpose(stacked).astype(jnp.bfloat16)


def turn(at, queries):
    tok = queries.shape[0]
    return pl.pallas_call(
        turn_kernel,
        out_shape=[jax.ShapeDtypeStruct((D, HEADS * tok), jnp.bfloat16)] * 4,
        in_specs=[SMEM, VMEM],
        out_specs=[VMEM] * 4,
        compiler_params=params(),
        name="turn_queries",
    )(at, queries)


def place_kernel(at_ref, *refs):
    out_ref = refs[4]
    width = HEADS * D
    for k in range(4):
        head = lax.rem(at_ref[0] + k, 4)
        out_ref[:, pl.ds(pl.multiple_of(head * width, width), width)] = refs[k][...]


def place(at, blocks):
    tok = blocks[0].shape[0]
    return pl.pallas_call(
        place_kernel,
        out_shape=jax.ShapeDtypeStruct((tok, 4 * HEADS * D), jnp.bfloat16),
        in_specs=[SMEM] + [VMEM] * 4,
        out_specs=VMEM,
        compiler_params=params(),
        name="place_heads",
    )(at, *blocks)


def make_attend(first_unit, units, piece_rows, span_rows, count, width):
    tiles = 2 * width // 256
    tok = span_rows // 2
    padded = count + 2 * NB

    def kernel(table, qa, qb, kv, own_ref, other_ref, acc, m, l, s0, s1, t0, t1):
        at_tab, at_span, at_full, at_q = 0, padded, 2 * padded, 2 * padded + 16
        koff, near, away = table[2 * padded + 24], table[2 * padded + 25], table[2 * padded + 26]

        def q_tile(j, t):
            lo = t * 256
            if lo + 256 <= width:
                return qa[j, :, lo : lo + 256]
            if lo >= width:
                return qb[j, :, lo - width : lo - width + 256]
            return jnp.concatenate([qa[j, :, lo:], qb[j, :, : 256 - (width - lo)]], axis=1)

        def rows_of(base):
            return [
                pl.ds(pl.multiple_of(table[at_tab + base + i] * piece_rows, 16), piece_rows) for i in range(NB)
            ]

        def score(j, base, s_ref, top_ref):
            keys = jnp.concatenate([kv[r, 0:D] for r in rows_of(base)], axis=0)
            for t in range(tiles):
                cs = pl.ds(t * 256, 256)
                s = jnp.dot(keys, q_tile(j, t), preferred_element_type=jnp.float32)
                s_ref[:, cs] = s
                top_ref[:, cs] = jnp.max(s, axis=0, keepdims=True)

        def absorb(j, base, s_ref, top_ref, masked):
            vals = jnp.concatenate([kv[r, D : 2 * D] for r in rows_of(base)], axis=0)
            if masked:
                within = lax.broadcasted_iota(jnp.int32, (piece_rows, 256), 0) + koff
                kpos = jnp.concatenate(
                    [within + table[at_span + base + i] * span_rows for i in range(NB)], axis=0
                )
            for t in range(tiles):
                cs = pl.ds(t * 256, 256)
                s = s_ref[:, cs]
                if masked:
                    col = lax.broadcasted_iota(jnp.int32, (1, 256), 1) + t * 256
                    qpos = lax.rem(col, tok) + jnp.where(col < width, near, away) + table[at_q + j] * span_rows
                    ok = kpos <= qpos
                    s = jnp.where(ok, s, LOW)
                    top = jnp.max(s, axis=0, keepdims=True)
                else:
                    top = top_ref[:, cs]
                m_old = m[:, cs]
                m_new = jnp.maximum(m_old, top * SCALE)
                alpha = jnp.exp2(m_old - m_new)
                p = jnp.exp2(s * SCALE - m_new)
                if masked:
                    p = jnp.where(ok, p, 0.0)
                l[:, cs] = l[:, cs] * alpha + jnp.sum(p, axis=0, keepdims=True)
                m[:, cs] = m_new
                pv = lax.dot_general(
                    vals, p.astype(jnp.bfloat16), (((0,), (0,)), ((), ())), preferred_element_type=jnp.float32
                )
                acc[:, cs] = acc[:, cs] * alpha + pv

        def one_span(u, carry):
            j = u + first_unit
            acc[...] = jnp.zeros(acc.shape, jnp.float32)
            m[...] = jnp.full(m.shape, LOW, jnp.float32)
            l[...] = jnp.zeros(l.shape, jnp.float32)
            full = table[at_full + j] // NB
            score(j, 0, s0, t0)

            def step(i, c):
                base = i * (2 * NB)
                score(j, base + NB, s1, t1)
                absorb(j, base, s0, t0, False)
                score(j, base + 2 * NB, s0, t0)
                absorb(j, base + NB, s1, t1, False)
                return c

            lax.fori_loop(0, full // 2, step, 0)
            odd = full % 2 == 1

            @pl.when(odd)
            def _():
                score(j, full * NB, s1, t1)
                absorb(j, full * NB - NB, s0, t0, False)
                absorb(j, full * NB, s1, t1, True)

            @pl.when(jnp.logical_not(odd))
            def _():
                absorb(j, full * NB, s0, t0, True)

            total = l[...]
            seen = total > 0.0
            safe = jnp.where(seen, total, 1.0)
            lse = jnp.where(seen, m[...] + jnp.log2(safe), LOW)
            inv = 1.0 / safe
            hi = lse.astype(jnp.bfloat16).astype(jnp.float32)
            mid = (lse - hi).astype(jnp.bfloat16).astype(jnp.float32)
            stat = jnp.concatenate([hi, mid, lse - hi - mid, jnp.zeros((5, 2 * width), jnp.float32)], axis=0)
            stat = stat.astype(jnp.bfloat16)
            for ref, lo in ((own_ref, 0), (other_ref, width)):
                cs = pl.ds(lo, width)
                ref[u, 0:D] = (acc[:, cs] * inv[:, lo : lo + width]).astype(jnp.bfloat16)
                ref[u, D:ROWS_O] = stat[:, lo : lo + width]
            return carry

        lax.fori_loop(0, units, one_span, 0)

    return kernel


def attend(table, qa, qb, kv, piece_rows, span_rows, first, units):
    width = qa.shape[2]
    count = kv.shape[0] // piece_rows
    wide = 2 * width
    flops = 2 * 2 * units * wide * D * kv.shape[0] // 2
    return pl.pallas_call(
        make_attend(first, units, piece_rows, span_rows, count, width),
        out_shape=[jax.ShapeDtypeStruct((units, ROWS_O, width), jnp.bfloat16)] * 2,
        in_specs=[SMEM] + [VMEM] * 3,
        out_specs=[VMEM] * 2,
        scratch_shapes=[
            pltpu.VMEM((D, wide), jnp.float32),
            pltpu.VMEM((1, wide), jnp.float32),
            pltpu.VMEM((1, wide), jnp.float32),
            pltpu.VMEM((NB * piece_rows, wide), jnp.float32),
            pltpu.VMEM((NB * piece_rows, wide), jnp.float32),
            pltpu.VMEM((1, wide), jnp.float32),
            pltpu.VMEM((1, wide), jnp.float32),
        ],
        compiler_params=params(),
        cost_estimate=pl.CostEstimate(flops=flops * 2, bytes_accessed=kv.size * 2, transcendentals=0),
    )(table, qa, qb, kv)


def weights_of(a, b):
    def lse(ref):
        s = ref[D : D + 8].astype(jnp.float32)
        return s[0:1] + s[1:2] + s[2:3]

    la, lb = lse(a), lse(b)
    top = jnp.maximum(la, lb)
    ea, eb = jnp.exp2(la - top), jnp.exp2(lb - top)
    total = ea + eb
    return ea / total, eb / total, top + jnp.log2(total)


def combine_kernel(a_ref, b_ref, keep_ref, send_ref):
    half = keep_ref.shape[0]
    for j in range(a_ref.shape[0]):
        wa, wb, lse = weights_of(a_ref[j], b_ref[j])
        mixed = a_ref[j, 0:D].astype(jnp.float32) * wa + b_ref[j, 0:D].astype(jnp.float32) * wb
        hi = lse.astype(jnp.bfloat16).astype(jnp.float32)
        mid = (lse - hi).astype(jnp.bfloat16).astype(jnp.float32)
        stat = jnp.concatenate([hi, mid, lse - hi - mid, jnp.zeros((5, lse.shape[1]), jnp.float32)], axis=0)
        ref = keep_ref if j < half else send_ref
        ref[j % half, 0:D] = mixed.astype(jnp.bfloat16)
        ref[j % half, D:ROWS_O] = stat.astype(jnp.bfloat16)


def combine(a, b):
    n = a.shape[0] // 2
    shape = jax.ShapeDtypeStruct((n,) + a.shape[1:], jnp.bfloat16)
    return pl.pallas_call(
        combine_kernel,
        out_shape=[shape, shape],
        in_specs=[VMEM] * 2,
        out_specs=[VMEM] * 2,
        compiler_params=params(),
        name="combine_cores",
    )(a, b)


def finish_kernel(a_ref, b_ref, *out_refs):
    tok = out_refs[0].shape[0]
    for j, out_ref in enumerate(out_refs):
        wa, wb, _ = weights_of(a_ref[j], b_ref[j])
        mixed = a_ref[j, 0:D].astype(jnp.float32) * wa + b_ref[j, 0:D].astype(jnp.float32) * wb
        rows = jnp.transpose(mixed).astype(jnp.bfloat16)
        for h in range(HEADS):
            out_ref[:, pl.ds(h * D, D)] = rows[h * tok : (h + 1) * tok]


def finish(a, b):
    tok = a.shape[2] // HEADS
    return pl.pallas_call(
        finish_kernel,
        out_shape=[jax.ShapeDtypeStruct((tok, HEADS * D), jnp.bfloat16)] * a.shape[0],
        in_specs=[VMEM] * 2,
        out_specs=[VMEM] * a.shape[0],
        compiler_params=params(),
        name="combine_chips",
    )(a, b)


def swap(x, axis):
    return lax.ppermute(x, axis, [(0, 1), (1, 0)])


def shift(x, k):
    return lax.ppermute(x, "zh", [(i, (i + k) % 4) for i in range(4)])


def exchange(x, axes):
    return lax.all_to_all(x, axes, split_axis=0, concat_axis=0, tiled=True)


def pick(values, index):
    slots = jnp.arange(values.shape[0], dtype=jnp.int32)
    return jnp.sum(jnp.where(slots[None, :] == index[:, None], values[None, :], 0), axis=1)


def per_device(queries, key_vectors, value_matrix, span_order):
    tok = queries.shape[0]
    pairs = span_order.shape[0]
    span_rows = 2 * tok
    piece = tok // 2
    yx = lax.axis_size("y") * lax.axis_size("x")
    zh, zl, c = (lax.axis_index(a).astype(jnp.int32) for a in ("zh", "zl", "c"))
    mine = lax.axis_index("y").astype(jnp.int32) * lax.axis_size("x") + lax.axis_index("x").astype(jnp.int32)
    at = jnp.stack([zh, zl])

    column = exchange(split_heads(key_vectors, value_matrix), ("zh", "zl"))
    blocks = turn(at, queries)
    spread = jnp.broadcast_to(column.reshape(1, 8 * piece, 2 * D), (yx, 8 * piece, 2 * D))
    spread, blocks = lax.optimization_barrier((spread, blocks))
    gathered = exchange(spread, ("y", "x"))
    gathered = gathered.reshape(yx * 8 * piece, 2 * D)

    got = [blocks[0]] + [shift(blocks[k], k) for k in range(1, 4)]
    far = swap(jnp.stack(got), "zl")
    q_near = jnp.stack([b for ks in GROUPS for b in [got[k] for k in ks] + [far[k] for k in ks]])
    q_far = swap(q_near, "c")

    order = span_order.astype(jnp.int32)
    span = jnp.arange(2 * pairs, dtype=jnp.int32)
    early = jnp.minimum(span, 2 * pairs - 1 - span)
    ids = jnp.arange(pairs, dtype=jnp.int32)
    pair = jnp.sum(jnp.where(order[None, :] == early[:, None], ids[None, :], 0), axis=1)
    tab = (pair % yx) * 8 + (pair // yx) * 2 + (span >= pairs)
    behind = (zh - jnp.asarray([k for ks in GROUPS for k in ks + ks], jnp.int32)) % 4
    other = jnp.asarray([f for ks in GROUPS for f in [0] * len(ks) + [1] * len(ks)], jnp.int32)
    here = pick(order, behind * yx + mine)
    q_span = jnp.where(zl == other, here, 2 * pairs - 1 - here)
    pad = jnp.zeros((2 * NB,), jnp.int32)
    scalars = jnp.stack([c * tok + zl * piece, c * tok, (1 - c) * tok])
    table = jnp.concatenate([tab, pad, span, pad + (1 << 16), q_span, q_span + 1, q_span, scalars])

    ends, first = {}, 0
    for ks in GROUPS:
        own, other = attend(table, q_near, q_far, gathered, piece, span_rows, first, 2 * len(ks))
        first += 2 * len(ks)
        keep, send = combine(own, swap(other, "c"))
        done = finish(keep, swap(send, "zl"))
        for i, k in enumerate(ks):
            ends[k] = done[i] if k == 0 else shift(done[i], 4 - k)
    return place(at, [ends[k] for k in range(4)])


def solution(mesh):
    finer = Mesh(mesh.devices.reshape(4, 4, 4, 2, 2), AXES)
    spec = P(AXES, None)
    return jax.shard_map(
        per_device, mesh=finer, in_specs=(spec, spec, spec, P()), out_specs=spec, check_vma=False
    )
```
